8 devices in a mesh: rep: 1 (over z), dp: 8 (over x, y, core).
Axes of the slice: x: 2, y: 2, z: 1, core: 2. Of those that a mesh axis runs over, the one named last changes fastest.
Arguments:
- g_w_gate: bfloat16 [8, 2, 512, 8192], P(('rep', 'dp'))
- g_w_up: bfloat16 [8, 2, 512, 8192], P(('rep', 'dp'))
- g_w_down: bfloat16 [8, 2, 8192, 512], P(('rep', 'dp'))
- w_gate: bfloat16 [2, 512, 8192], replicated
- w_up: bfloat16 [2, 512, 8192], replicated
- w_down: bfloat16 [2, 8192, 512], replicated
- m_w_gate: float32 [2, 512, 8192], P(None, 'dp')
- m_w_up: float32 [2, 512, 8192], P(None, 'dp')
- m_w_down: float32 [2, 8192, 512], P(None, 'dp')
- v_w_gate: float32 [2, 512, 8192], P(None, 'dp')
- v_w_up: float32 [2, 512, 8192], P(None, 'dp')
- v_w_down: float32 [2, 8192, 512], P(None, 'dp')
Outputs:
- output 1: bfloat16 [2, 512, 8192], P('rep')
- output 2: bfloat16 [2, 512, 8192], P('rep')
- output 3: bfloat16 [2, 8192, 512], P('rep')
- output 4: float32 [2, 512, 8192], P('rep', 'dp')
- output 5: float32 [2, 512, 8192], P('rep', 'dp')
- output 6: float32 [2, 8192, 512], P('rep', 'dp')
- output 7: float32 [2, 512, 8192], P('rep', 'dp')
- output 8: float32 [2, 512, 8192], P('rep', 'dp')
- output 9: float32 [2, 8192, 512], P('rep', 'dp')
All inputs are finite; a program needn't handle non-finite values.
Results may differ from the reference program's by a relative error of at most 0.022.
Values are sent between devices in bfloat16 or wider.
A program may use at most 2 GiB of HBM per device.

```python
import jax
import jax.numpy as jnp
from jax import lax

DEVICES = 8
D = 512
FF = 8192
LAYERS = 2
NAMES = ("w_gate", "w_up", "w_down")
SHAPES = {"w_gate": (LAYERS, D, FF), "w_up": (LAYERS, D, FF), "w_down": (LAYERS, FF, D)}


def setup_inputs(seed: int = 0, part: int = 0) -> dict:
    kz, *keys = jax.random.split(jax.random.key(seed), 1 + 5 * len(NAMES))
    loud = 2.0 ** jax.random.uniform(kz, (), jnp.float32, -1.0, 1.0)
    drawn = {}
    for name, key, both in zip(NAMES, keys[:3], keys[3:6], strict=True):
        own = jax.random.normal(jax.random.fold_in(key, part), (DEVICES, *SHAPES[name]), jnp.float32)
        shared = jax.random.normal(jax.random.fold_in(both, part), SHAPES[name], jnp.float32)
        drawn["g_" + name] = (loud * (0.7 * shared / DEVICES + 0.7 * own * DEVICES**-0.5)).astype(jnp.bfloat16)
    for name, key in zip(NAMES, keys[6:9], strict=True):
        drawn[name] = (jax.random.normal(key, SHAPES[name], jnp.float32) * SHAPES[name][1] ** -0.5).astype(jnp.bfloat16)
    for name, key in zip(NAMES, keys[9:12], strict=True):
        drawn["m_" + name] = loud * 0.5 * jax.random.normal(key, SHAPES[name], jnp.float32)
    for name, key in zip(NAMES, keys[12:15], strict=True):
        drawn["v_" + name] = loud * loud * jax.random.uniform(key, SHAPES[name], jnp.float32, 0.5, 1.5)
    return drawn


def adamw(w, m, v, g):
    m = 0.9 * m + 0.1 * g
    v = 0.95 * v + 0.05 * g * g
    step = m * lax.rsqrt(v + 1e-8) + 0.1 * w
    return (w - 0.02 * step).astype(jnp.bfloat16), m, v


def reference(g_w_gate, g_w_up, g_w_down, w_gate, w_up, w_down, m_w_gate, m_w_up, m_w_down, v_w_gate, v_w_up, v_w_down):
    def total(terms):
        return lax.scan(lambda so_far, term: (so_far + term.astype(jnp.float32), None), jnp.zeros(terms.shape[1:], jnp.float32), terms)[0]

    gradients = [total(terms).astype(jnp.bfloat16).astype(jnp.float32) for terms in (g_w_gate, g_w_up, g_w_down)]
    new = [
        adamw(w.astype(jnp.float32), m, v, g)
        for w, m, v, g in zip((w_gate, w_up, w_down), (m_w_gate, m_w_up, m_w_down), (v_w_gate, v_w_up, v_w_down), gradients, strict=True)
    ]
    return tuple(one[which] for which in range(3) for one in new)
```

```python
import functools

import jax
import jax.numpy as jnp
from jax import lax
from jax.experimental import pallas as pl
from jax.experimental.pallas import tpu as pltpu
from jax.sharding import PartitionSpec as P

MESH = pl.DeviceIdType.MESH
F32, BF16 = jnp.float32, jnp.bfloat16
STEPS = ((0, 0), (1, 0), (0, 1), (1, 1), (2, 0), (2, 1))
ROWS = ((32, 8192), (512, 512))
COLS = 512


def adamw(w, m, v, g):
    m = 0.9 * m + 0.1 * g
    v = 0.95 * v + 0.05 * g * g
    step = m * lax.rsqrt(v + 1e-8) + 0.1 * w
    return (w - 0.02 * step).astype(jnp.bfloat16), m, v


def tiles(shape, body):
    across = shape[1] // COLS

    def one(i, _):
        if across == 1:
            r, c = i, 0
            body((pl.ds(pl.multiple_of(r * 16, 16), 16), pl.ds(0, COLS)))
        else:
            r, c = i // across, i % across
            body((pl.ds(pl.multiple_of(r * 16, 16), 16), pl.ds(pl.multiple_of(c * COLS, COLS), COLS)))
        return _

    lax.fori_loop(0, shape[0] // 16 * across, one, 0, unroll=2)


def kernel(*refs):
    it = iter(refs)

    def take(n):
        return [next(it) for _ in range(n)]

    g, w, m, v = take(3), take(3), take(3), take(3)
    w_out, g_out = take(3), take(3)
    pt, r1, r2, own, w_in, m_in, v_in = (take(2) for _ in range(7))
    d2d_s, d2d_r, l1_s, l1_r, l2_s, l2_r, ag_s, ag_r, agc_s, agc_r = take(10)
    own_sem, opt_sem, out_sem = take(3)

    me = lax.axis_index("dp")
    core = lax.rem(me, 2)
    y = lax.rem(me // 2, 2)
    x = me // 4

    def dev(bx, by, bc):
        return bx * 4 + by * 2 + bc

    partner = dev(x, y, 1 - core)
    nx, ny = dev(1 - x, y, core), dev(x, 1 - y, core)
    first, second = (nx, ny), (ny, nx)

    def chip(colour, block):
        f, s = ((1, 0), (1, 1), (0, 1), (0, 0))[block]
        fx, fy = (f, s) if colour == 0 else (s, f)
        return (1 - x if fx else x), (1 - y if fy else y)

    def kind(step):
        return 1 if STEPS[step][0] == 2 else 0

    def at(step):
        return step - 4 if kind(step) else step

    def region(ref, step, colour, device):
        n = ROWS[kind(step)][0]
        start = pl.multiple_of(device * (2 * n) + colour * n, n)
        return ref.at[STEPS[step][1], pl.ds(start, n)]

    def block_of(ref, step, colour, block, bc):
        return region(ref, step, colour, dev(*chip(colour, block), bc))

    def remote(src, dst, ss, rs, device):
        return pltpu.make_async_remote_copy(src, dst, ss, rs, device_id={"dp": device}, device_id_type=MESH)

    def load_own(step, colour, block):
        return pltpu.make_async_copy(
            block_of(g[STEPS[step][0]], step, colour, block, core), own[kind(step)].at[colour, block], own_sem.at[kind(step), colour, block]
        )

    def load_opt(step, colour):
        q, (which, layer), k = kind(step), STEPS[step], ROWS[kind(step)][0]
        here = pl.ds(colour * k, k)
        return (
            pltpu.make_async_copy(region(w[which], step, colour, me), w_in[q].at[colour], opt_sem.at[q, colour, 0]),
            pltpu.make_async_copy(m[which].at[layer, here], m_in[q].at[colour], opt_sem.at[q, colour, 1]),
            pltpu.make_async_copy(v[which].at[layer, here], v_in[q].at[colour], opt_sem.at[q, colour, 2]),
        )

    def d2d(step, colour, block):
        return remote(
            block_of(g[STEPS[step][0]], step, colour, block, 1 - core),
            pt[kind(step)].at[at(step), colour, block],
            d2d_s.at[step, colour, block],
            d2d_r.at[step, colour, block],
            partner,
        )

    def sum1(step, colour, block):
        q, i = kind(step), at(step)
        return remote(
            pt[q].at[i, colour, block], r1[q].at[i, colour, block], l1_s.at[step, colour, block], l1_r.at[step, colour, block], first[colour]
        )

    def sum2(step, colour):
        q, i = kind(step), at(step)
        return remote(r1[q].at[i, colour, 1], r2[q].at[i, colour], l2_s.at[step, colour], l2_r.at[step, colour], second[colour])

    def out_block(step, colour, block):
        return block_of(w_out[STEPS[step][0]], step, colour, block, core)

    def keep(step, colour):
        q, i, (which, layer), k = kind(step), at(step), STEPS[step], ROWS[kind(step)][0]
        return (
            pltpu.make_async_copy(r2[q].at[i, colour], out_block(step, colour, 3), out_sem.at[step, colour, 0]),
            pltpu.make_async_copy(r1[q].at[i, colour, 0], g_out[which].at[layer, pl.ds(colour * k, k)], out_sem.at[step, colour, 1]),
        )

    def gather(step, colour, hop):
        q, i = kind(step), at(step)
        src = out_block(step, colour, 2) if hop == 2 else r2[q].at[i, colour]
        dst = out_block(step, colour, 2 if hop == 2 else 3)
        return remote(src, dst, ag_s.at[step, colour, hop], ag_r.at[step, colour, hop], second[colour] if hop == 0 else first[colour])

    def across(step, colour, block):
        q, i = kind(step), at(step)
        src = r2[q].at[i, colour] if block == 3 else out_block(step, colour, block)
        return remote(src, out_block(step, colour, block), agc_s.at[step, colour, block], agc_r.at[step, colour, block], partner)

    def stage1(step):
        for block in (0, 1):
            for colour in (0, 1):
                q, i = kind(step), at(step)
                load_own(step, colour, block).wait()
                d2d(step, colour, block).wait_recv()
                a, b = own[q].at[colour, block], pt[q].at[i, colour, block]

                def add(t, a=a, b=b):
                    b[t] = (a[t].astype(F32) + b[t].astype(F32)).astype(BF16)

                tiles(ROWS[q], add)
                sum1(step, colour, block).start()
                if step + 1 < len(STEPS):
                    load_own(step + 1, colour, block).start()
        for block, later in ((0, 2), (1, 2), (2, 0), (3, 0)):
            for colour in (0, 1):
                if step + later < len(STEPS):
                    d2d(step + later, colour, block).start()

    def stage2(step):
        for colour in (0, 1):
            q, i = kind(step), at(step)
            load_own(step, colour, 2).wait()
            d2d(step, colour, 2).wait_recv()
            sum1(step, colour, 1).wait_recv()
            a, b, c = own[q].at[colour, 2], pt[q].at[i, colour, 2], r1[q].at[i, colour, 1]

            def add(t, a=a, b=b, c=c):
                c[t] = (a[t].astype(F32) + b[t].astype(F32) + c[t].astype(F32)).astype(BF16)

            tiles(ROWS[q], add)
            sum2(step, colour).start()
            if step + 1 < len(STEPS):
                load_own(step + 1, colour, 2).start()

    def stage3(step):
        for colour in (0, 1):
            q, i = kind(step), at(step)
            load_own(step, colour, 3).wait()
            for c in load_opt(step, colour):
                c.wait()
            d2d(step, colour, 3).wait_recv()
            sum1(step, colour, 0).wait_recv()
            sum2(step, colour).wait_recv()
            a, b, c, d = own[q].at[colour, 3], pt[q].at[i, colour, 3], r1[q].at[i, colour, 0], r2[q].at[i, colour]
            wr, mr, vr = w_in[q].at[colour], m_in[q].at[colour], v_in[q].at[colour]

            def update(t, a=a, b=b, c=c, d=d, wr=wr, mr=mr, vr=vr):
                grad = (a[t].astype(F32) + b[t].astype(F32) + (c[t].astype(F32) + d[t].astype(F32))).astype(BF16)
                c[t] = grad
                d[t] = adamw(wr[t].astype(F32), mr[t], vr[t], grad.astype(F32))[0]

            tiles(ROWS[q], update)
            gather(step, colour, 0).start()
            gather(step, colour, 1).start()
            across(step, colour, 3).start()
            for c in keep(step, colour):
                c.start()
            if step + 1 < len(STEPS):
                load_own(step + 1, colour, 3).start()
                for c in load_opt(step + 1, colour):
                    c.start()

    def stage4(step):
        for colour in (0, 1):
            gather(step, colour, 0).wait_recv()
            gather(step, colour, 2).start()
            across(step, colour, 2).start()

    def stage5(step):
        for hop, block in ((1, 0), (2, 1)):
            for colour in (0, 1):
                gather(step, colour, hop).wait_recv()
                across(step, colour, block).start()

    def finish():
        for step in range(len(STEPS)):
            for colour in (0, 1):
                for block in range(4):
                    d2d(step, colour, block).wait_send()
                    across(step, colour, block).wait()
                for block in (0, 1):
                    sum1(step, colour, block).wait_send()
                sum2(step, colour).wait_send()
                for hop in range(3):
                    gather(step, colour, hop).wait_send()
                for c in keep(step, colour):
                    c.wait()

    for block in range(4):
        for colour in (0, 1):
            load_own(0, colour, block).start()
    for colour in (0, 1):
        for c in load_opt(0, colour):
            c.start()
    barrier = pltpu.get_barrier_semaphore()
    for other in (partner, nx, ny):
        pl.semaphore_signal(barrier, inc=1, device_id={"dp": other}, device_id_type=MESH)
    pl.semaphore_wait(barrier, 3)
    for step in (0, 1):
        for block in (0, 1):
            for colour in (0, 1):
                d2d(step, colour, block).start()

    for stage, step in ORDER:
        (stage1, stage2, stage3, stage4, stage5)[stage - 1](step)
    finish()


ORDER = (
    (1, 0), (1, 1), (1, 2), (2, 0), (1, 3), (2, 1), (1, 4), (2, 2), (1, 5), (3, 0), (2, 3), (3, 1), (2, 4), (3, 2), (2, 5), (3, 3),
    (4, 0), (3, 4), (4, 1), (3, 5), (4, 2), (5, 0), (4, 3), (5, 1), (4, 4), (5, 2), (4, 5), (5, 3), (5, 4), (5, 5),
)


def solution(mesh):
    def step(*arrays):
        terms, weights, m, v = (arrays[i : i + 3] for i in (0, 3, 6, 9))
        terms = [t[0] for t in terms]
        any_, dma = pl.BlockSpec(memory_space=pl.ANY), pltpu.SemaphoreType.DMA
        n = len(STEPS)

        def bufs(dtype, *lead):
            return [pltpu.VMEM((*(k[q] if isinstance(k, tuple) else k for k in lead), *ROWS[q]), dtype) for q in (0, 1)]

        slots = (4, 2)
        outs = pl.pallas_call(
            kernel,
            out_shape=[jax.ShapeDtypeStruct(w.shape, BF16) for w in weights] + [jax.ShapeDtypeStruct(one.shape, BF16) for one in m],
            in_specs=[any_] * 12,
            out_specs=[any_] * 6,
            scratch_shapes=[
                *bufs(BF16, slots, 2, 4),
                *bufs(BF16, slots, 2, 2),
                *bufs(BF16, slots, 2),
                *bufs(BF16, 2, 4),
                *bufs(BF16, 2),
                *bufs(F32, 2),
                *bufs(F32, 2),
                dma((n, 2, 4)), dma((n, 2, 4)),
                dma((n, 2, 2)), dma((n, 2, 2)),
                dma((n, 2)), dma((n, 2)),
                dma((n, 2, 3)), dma((n, 2, 3)),
                dma((n, 2, 4)), dma((n, 2, 4)),
                dma((2, 2, 4)), dma((2, 2, 3)), dma((n, 2, 2)),
            ],
            compiler_params=pltpu.CompilerParams(collective_id=0, has_side_effects=True, vmem_limit_bytes=67043328),
        )(*terms, *weights, *m, *v)
        whole, grads = outs[:3], [one.astype(F32) for one in outs[3:]]
        new_m = [0.9 * one + 0.1 * grad for one, grad in zip(m, grads, strict=True)]
        new_v = [0.95 * one + 0.05 * grad * grad for one, grad in zip(v, grads, strict=True)]
        return (*whole, *new_m, *new_v)

    all_of, cut = P(None, None, None), P(None, "dp", None)
    return jax.shard_map(
        step,
        mesh=mesh,
        in_specs=(P(("rep", "dp"), None, None, None),) * 3 + (all_of,) * 3 + (cut,) * 6,
        out_specs=(P("rep", None, None),) * 3 + (P("rep", "dp", None),) * 6,
        check_vma=False,
    )
```
